32 devices in a mesh: band: 2 (over y), grid: 16 (over z, x, core).
Axes of the slice: x: 2, y: 2, z: 4, core: 2. Of those that a mesh axis runs over, the one named last changes fastest.
Arguments:
- orbitals: bfloat16 [2048, 32768], P('band', 'grid'), as said below
- projectors: bfloat16 [2048, 32768], P('band', 'grid'), may hold values from -0.0234375 to 0.0234375
Outputs:
- result: bfloat16 [2048, 32768], P('band', 'grid')
- energies: float32 [2048], P('band')
The draws below stay inside these ranges and needn't reach their ends.
Inputs may be any that keep to these rules, and one draw needn't show every extreme that they name: The orbitals are real-valued.
All inputs are finite; a program needn't handle non-finite values.
Results may differ from the reference program's by a relative error of at most 0.0049.
Values may be sent and summed in bfloat16 or wider, within the bound.
A program may use at most 64 MiB of HBM per device.

```python
import jax
import jax.numpy as jnp
from jax import lax

NB = 2048
NG = 32768


def draw_orbitals(key, part):
    k_main = jax.random.fold_in(key, 11)
    k_rough = jax.random.fold_in(key, 12)
    place = jnp.arange(NG, dtype=jnp.float32) / (NG - 1)
    rising = 0.6 + 1.2 * place
    rough = jax.random.uniform(k_rough, (1, NG), jnp.float32, 0.5, 1.5)
    values = jax.random.normal(k_main, (NB, NG), jnp.float32)
    return (values * rising[None, :] * rough).astype(jnp.bfloat16)


def steps_of(rng, shape, pieces, smallest, top_value):
    factor_of = 1.0
    for dim, shards_of in pieces:
        steps = jax.random.uniform(jax.random.fold_in(jax.random.fold_in(rng, 6), dim), (shards_of,), jnp.float32, smallest / len(pieces), top_value / len(pieces))
        factor_of = factor_of * jnp.repeat(jnp.exp(steps), shape[dim] // shards_of).reshape((-1,) + (1,) * (len(shape) - 1 - dim))
    return factor_of


def normal_values(rng, dims, scale, limit, shards=(), kind=jnp.bfloat16):
    array = jax.random.normal(rng, dims, jnp.float32) * scale
    if len(shards) > 0:
        array = steps_of(rng, dims, shards, -0.22, 0.18) * array
    return jnp.clip(array, min=-limit, max=limit).astype(kind)


def setup_inputs(seed: int = 0) -> dict:
    splits = jax.random.split(jax.random.key(seed), 3)
    return {
        "orbitals": draw_orbitals(jax.random.fold_in(splits[2], 71), 0),
        "projectors": normal_values(splits[1], (NB, NG), (2 * NG) ** -0.5, 0.0234375, ((0, 2), (1, 16))),
    }


def intersections(projectors, state):
    return jnp.dot(projectors.astype(jnp.float32), state.astype(jnp.float32).T, preferred_element_type=jnp.float32)


def update(projectors, state, rounded):
    widened = lax.optimization_barrier(rounded).astype(jnp.float32)
    return state.astype(jnp.float32) - jnp.dot(widened.T, projectors.astype(jnp.float32), preferred_element_type=jnp.float32)


def reference(orbitals, projectors):
    first = intersections(projectors, orbitals)
    first_b = first.astype(jnp.bfloat16)
    middle = update(projectors, orbitals, first_b).astype(jnp.bfloat16)
    second = intersections(projectors, middle)
    second_b = second.astype(jnp.bfloat16)
    result = update(projectors, middle, second_b).astype(jnp.bfloat16)
    wide = middle.astype(jnp.float32)
    norm = jnp.sum(wide * wide, axis=1)
    numer = jnp.sum(second * lax.optimization_barrier(second_b).astype(jnp.float32), axis=0)
    energies = (2.0 * NG / NB) * numer / norm
    return result, energies
```

```python
import jax
import jax.numpy as jnp
from jax import lax
from jax.sharding import PartitionSpec as P

LEAST_ROWS = 16
MOST_PIECES = 2


def rows_by_rows(left, right):
    return lax.dot_general(
        left, right, (((1,), (1,)), ((), ())), preferred_element_type=jnp.float32
    )


def apply_terms(rounded, rows):
    return lax.dot_general(
        rounded, rows, (((0,), (0,)), ((), ())), preferred_element_type=jnp.float32
    )


def stages(grids):
    pair = 2 if grids % 2 == 0 else 1
    rest = grids // pair
    near = 1
    while near * 2 * near * 2 <= rest and rest % (near * 2) == 0:
        near *= 2
    pair_part, near_part, far_part = (1, pair), (pair, near), (pair * near, rest // near)
    return ([pair_part, near_part, far_part], [pair_part, far_part, near_part])


def shifted(block, stride, size, by, grids):
    moves = []
    for i in range(grids):
        at = i // stride % size
        moves.append((i, i + ((at + by) % size - at) * stride))
    return lax.ppermute(block, "grid", moves)


def scatter_sum(terms, order, grids):
    me = lax.axis_index("grid")
    total = terms
    for stride, size in order:
        if size == 1:
            continue
        at = me // stride % size
        pieces, rows, columns = total.shape
        blocks = total.astype(jnp.bfloat16).reshape(pieces, size, rows // size, columns)

        def block_of(place):
            return lax.dynamic_index_in_dim(blocks, place % size, axis=1, keepdims=False)

        come = [shifted(block_of(at + by), stride, size, by, grids) for by in range(1, size)]
        total = block_of(at).astype(jnp.float32)
        for block in come:
            total = total + block.astype(jnp.float32)
    return total.astype(jnp.float32)


def gather(share, order, grids):
    me = lax.axis_index("grid")
    for stride, size in reversed(order):
        if size == 1:
            continue
        at = me // stride % size
        pieces, rows, columns = share.shape
        out = jnp.zeros((pieces, size, rows, columns), share.dtype)
        out = lax.dynamic_update_slice_in_dim(out, share[:, None], at, axis=1)
        for by in range(1, size):
            block = shifted(share, stride, size, by, grids)
            out = lax.dynamic_update_slice_in_dim(out, block[:, None], (at - by + size) % size, axis=1)
        share = out.reshape(pieces, size * rows, columns)
    return share


def sum_over_grid(values, grids):
    for stride, size in stages(grids)[0]:
        come = [shifted(values, stride, size, by, grids) for by in range(1, size)]
        for block in come:
            values = values + block
    return values


def per_device(orbitals, projectors):
    bands, grids = lax.axis_size("band"), lax.axis_size("grid")
    rows, points = projectors.shape
    total_bands, total_points = rows * bands, points * grids
    split = max(1, min(MOST_PIECES, rows // (LEAST_ROWS * grids)))
    height = rows // split
    share_rows = height // grids
    orders = stages(grids)

    def band_shift(block, by):
        return lax.ppermute(block, "band", [(i, (i - by) % bands) for i in range(bands)])

    steps = [[projectors[p * height : (p + 1) * height] for p in range(split)]]
    for d in range(1, bands):
        steps.append([band_shift(piece, 1) for piece in steps[-1]])

    both = jnp.concatenate([orbitals, projectors], axis=0)
    kinds = [[p for p in range(split) if p % 2 == k] for k in range(2)]

    def by_kind(act):
        found = [None] * split
        for order, members in zip(orders, kinds):
            if members:
                result = act(order, members)
                for place, p in enumerate(members):
                    found[p] = result[place]
        return found

    first, gram, first_b = [], [], []
    for d in range(bands):
        if d == 0:
            terms = rows_by_rows(projectors, both).astype(jnp.bfloat16).reshape(split, height, -1)
            shares = by_kind(
                lambda order, members: scatter_sum(
                    jnp.stack([terms[p] for p in members]), order, grids
                )
            )
        else:
            shares = []
            for p, piece in enumerate(steps[d]):
                terms = rows_by_rows(piece, both).astype(jnp.bfloat16)[None]
                shares.append(scatter_sum(terms, orders[p % 2], grids)[0])
        share = jnp.stack(shares)
        first.append(share[:, :, :rows])
        gram.append(share[:, :, rows:].astype(jnp.bfloat16))
        rounded = first[-1].astype(jnp.bfloat16)
        first_b.append(
            by_kind(
                lambda order, members: gather(
                    jnp.stack([rounded[p] for p in members]), order, grids
                )
            )
        )
    whole = jnp.concatenate([piece for step in steps for piece in step], axis=0)
    whole_first = jnp.concatenate([piece for step in first_b for piece in step], axis=0)

    columns = [jnp.stack(gram)]
    for by in range(1, bands):
        come = band_shift(columns[0], by)
        columns.append(jnp.roll(come, by, axis=0))
    products = jnp.concatenate(columns, axis=-1).reshape(-1, total_bands)
    share_first = jnp.stack(first).reshape(-1, rows)
    share_second = share_first - jnp.dot(
        products, whole_first, preferred_element_type=jnp.float32
    )
    share_b = share_second.astype(jnp.bfloat16)
    numer = jnp.sum(share_second * share_b.astype(jnp.float32), axis=0)

    parts_b = share_b.reshape(bands, split, share_rows, rows)
    found = by_kind(
        lambda order, members: jnp.stack(
            jnp.split(
                gather(
                    jnp.concatenate([parts_b[:, p] for p in members], axis=0), order, grids
                ),
                len(members),
            )
        )
    )
    second_b = jnp.stack(found, axis=1).reshape(total_bands, rows)

    middle = (orbitals.astype(jnp.float32) - apply_terms(whole_first, whole)).astype(jnp.bfloat16)
    widened = middle.astype(jnp.float32)
    norm = jnp.sum(widened * widened, axis=1)
    numer, norm = sum_over_grid(jnp.stack([numer, norm]), grids)
    result = (widened - apply_terms(second_b, whole)).astype(jnp.bfloat16)
    energies = 2.0 * total_points / total_bands * numer / norm
    return (result, energies)


def solution(mesh):
    in_specs = (P("band", "grid"), P("band", "grid"))
    out_specs = (P("band", "grid"), P("band"))
    return jax.shard_map(
        per_device, mesh=mesh, in_specs=in_specs, out_specs=out_specs, check_vma=False
    )
```
